32 devices in a mesh: dp: 4 (over x, core), expert: 4 (over z), etp: 2 (over y).
Axes of the slice: x: 2, y: 2, z: 4, core: 2. Of those that a mesh axis runs over, the one named last changes fastest.
Arguments:
- tokens: bfloat16 [4096, 3072], P(('dp', 'expert'), 'etp'), parts along dimension 0, may hold values from -6 to 6
- experts: int32 [4096, 2], P(('dp', 'expert')), parts along dimension 0, may hold values from 0 to 3, all different within a row; in each aligned block of 256 rows (0 to 255, 256 to 511, ...) at most 176 rows name the same one
- mixing: float32 [4096, 2], P(('dp', 'expert')), parts along dimension 0, may hold values from 0.2 to 1
- up_weight: bfloat16 [4, 3072, 8192], P('expert', None, 'etp'), may hold values from -0.109375 to 0.109375
- down_weight: bfloat16 [4, 8192, 3072], P('expert', 'etp'), may hold values from -0.0625 to 0.0625
Outputs:
- mixed: bfloat16 [4096, 3072], P(('dp', 'expert'), 'etp'), parts along dimension 0
The draws below stay inside these ranges and needn't reach their ends.
There are 4 independent parts, one for each index of `dp`. The reference program is written for one: setup_inputs(seed, part) draws one part's arguments, and reference() takes and returns one part's arrays. A program takes and returns all parts, laid end to end along the dimension named above; an argument that names none is the same for every part. Nothing has to cross between parts.
Inputs may be any that keep to these rules, and one draw needn't show every extreme that they name: Each row names two different experts. In the rows of one index of expert (aligned blocks of 256 rows) no expert is named more than 176 times, a bound that some block reaches.
All inputs are finite; a program needn't handle non-finite values.
Results may differ from the reference program's by a relative error of at most 0.0078.
Values may be sent and summed in bfloat16 or wider, within the bound.
A program may use at most 128 MiB of HBM per device.

```python
import math
import jax
import jax.numpy as jnp
import numpy as np
from jax import lax

D = 3072
FF = 8192
TOK_DEV = 256
E = 4
CAP = 176
TOKENS = 1024


def shard_levels(own_key, shape, pieces, low, high):
    factor_of, own = 1.0, jax.random.fold_in(own_key, 6)
    for position, parts in pieces:
        draws = jnp.exp(jax.random.uniform(jax.random.fold_in(own, position), (parts,), jnp.float32, low / len(pieces), high / len(pieces)))
        factor_of = factor_of * jnp.repeat(draws, shape[position] // parts).reshape([-1 if axis == position else 1 for axis in range(len(shape))])
    return factor_of


def deal_out(stream_key, own, number, rows, amount, top, most, skew):
    ranking = jax.random.permutation(stream_key, amount)
    packed, usual = shares(amount, rows * top, most, skew, True), shares(amount, rows * top, most, skew, False)
    places = jnp.arange(amount)

    def named(lengths, offset_by):
        used = int((lengths > 0).sum())
        fixed = max(1, used // 4)
        moved = fixed + (places - fixed + offset_by * (used - fixed)) % max(1, amount - fixed)
        return jnp.zeros((amount,), jnp.int32).at[ranking[jnp.where(places < fixed, places, moved)]].set(jnp.asarray(lengths, jnp.int32))

    lengths = jnp.where(number % 4 == 0, named(packed, number // 4), named(usual, number - number // 4 - 1))
    mixed = jax.random.permutation(jax.random.fold_in(own, 3), amount)
    giver, sink = mixed[0:amount // 2 * 2:2], mixed[1:amount // 2 * 2:2]
    room = jnp.minimum(lengths[giver] - 1, most - lengths[sink]) // 2
    room = jnp.where((giver == ranking[0]) | (sink == ranking[0]) | (lengths[sink] == 0), 0, jnp.maximum(room, 0))
    moved = jax.random.randint(jax.random.fold_in(own, 4), (amount // 2,), 0, 1 << 20) % (room + 1)
    lengths = lengths.at[giver].add(-moved).at[sink].add(moved)
    members = jnp.searchsorted(jnp.cumsum(lengths), jnp.arange(rows * top), side="right").astype(jnp.int32)
    grid = members.reshape(top, rows).T
    grid = grid[jax.random.permutation(jax.random.fold_in(own, 1), rows)]
    offset_by = jax.random.randint(jax.random.fold_in(own, 2), (rows, 1), 0, top)
    return jnp.take_along_axis(grid, (jnp.arange(top)[None, :] + offset_by) % top, axis=1)


def shares(count, total, reach, skew, full):
    weights = [(1 << 20) // math.isqrt(grade ** skew) + 1 for grade in range(1, count + 1)]
    largest = reach if full else min(reach, max(-(-total // count), total * weights[0] // sum(weights)))
    least = 1 if total - largest >= count - 1 else 0
    holding, spare = [largest] + [least] * (count - 1), total - largest - least * (count - 1)
    while spare > 0:
        candidates = [i for i in range(1, count) if holding[i] < largest] or [i for i in range(1, count) if holding[i] < reach]
        whole, budget = sum([weights[i] for i in candidates]), spare
        for i in candidates:
            extra = min(reach - holding[i], max(1, budget * weights[i] // whole), spare)
            holding[i] = holding[i] + extra
            spare = spare - extra
    return np.array(holding)


def gaussian(key, extent, spread, reach, pieces=(), kind=jnp.bfloat16):
    entries = spread * jax.random.normal(key, extent, jnp.float32)
    if pieces:
        entries = entries * shard_levels(key, extent, pieces, -0.22, 0.18)
    return jnp.clip(entries, -reach, reach).astype(kind)


def setup_inputs(seed: int = 0, part: int = 0) -> dict:
    key_of = jax.random.split(jax.random.key(seed), 6)
    part_splits = jax.random.split(jax.random.fold_in(key_of[5], part), 6)
    tokens = gaussian(part_splits[0], (TOKENS, D), 1.0, 6.0, ((0, 4), (1, 2)))
    experts_keys = jax.random.split(jax.random.fold_in(part_splits[1], 1), TOKENS // TOK_DEV)
    experts_turns = jax.random.permutation(jax.random.fold_in(part_splits[1], 3), TOKENS // TOK_DEV)
    experts = jax.vmap(lambda own, number: deal_out(jax.random.fold_in(part_splits[1], 2), own, number, TOK_DEV, E, 2, CAP, 2))(experts_keys, experts_turns).reshape((TOKENS, 2))
    mixing = jnp.clip(0.2 + 0.8 * jax.random.uniform(part_splits[2], (TOKENS, 2), jnp.float32) ** shard_levels(part_splits[2], (TOKENS, 2), ((0, 4),), -0.2, 0.2), 0.2, 1.0)
    up_weight = gaussian(key_of[3], (E, D, FF), D ** -0.5, 0.109375, ((0, 4), (2, 2)))
    down_weight = gaussian(key_of[4], (E, FF, D), FF ** -0.5, 0.0625, ((0, 4), (1, 2)))
    return dict(tokens=tokens, experts=experts, mixing=mixing, up_weight=up_weight, down_weight=down_weight)


def reference(tokens, experts, mixing, up_weight, down_weight):
    flat_ids = experts.reshape(-1).astype(jnp.int32)
    assigned = flat_ids.shape[0]
    ordering = jnp.arange(assigned, dtype=jnp.int32)
    capacity = CAP * (TOKENS // TOK_DEV)
    flat_mix = mixing.reshape(-1)

    def one_expert(expert):
        sort_key = jnp.where(flat_ids == expert, 0, assigned).astype(jnp.int32) + ordering
        picked = jnp.argsort(sort_key)[:capacity].astype(jnp.int32)
        is_live = flat_ids[picked] == expert
        chosen_rows = tokens[picked // 2]
        up_proj = jnp.dot(chosen_rows, up_weight[expert], preferred_element_type=jnp.float32)
        hidden = jax.nn.silu(up_proj).astype(jnp.bfloat16)
        expert_out = jnp.dot(hidden, down_weight[expert], preferred_element_type=jnp.float32).astype(jnp.bfloat16)
        scaled = jnp.where(is_live, flat_mix[picked], jnp.zeros_like(flat_mix[picked]))
        return expert_out.astype(jnp.float32) * scaled[:, None], picked

    terms, picked = lax.map(one_expert, jnp.arange(E, dtype=jnp.int32))
    mixed = jnp.zeros((TOKENS, D), jnp.float32).at[(picked // 2).reshape(-1)].add(terms.reshape(-1, D))
    return mixed.astype(jnp.bfloat16)
```

```python
import jax
import jax.numpy as jnp
from jax import lax
from jax.sharding import PartitionSpec as P


def swap(x, axis, shift):
    count = lax.axis_size(axis)
    return lax.ppermute(x, axis, [(i, i ^ shift) for i in range(count)])


def slot_table(chosen, expert_count, capacity):
    flat_ids = chosen.reshape(-1)
    one_hot = (flat_ids[:, None] == jnp.arange(expert_count, dtype=jnp.int32)[None, :]).astype(
        jnp.int32
    )
    before = jnp.cumsum(one_hot, axis=0) - one_hot
    position = jnp.sum(before * one_hot, axis=1)
    return (flat_ids * capacity + position).reshape(chosen.shape)


def local(tokens, experts, mixing, up_weight, down_weight):
    tok_rows = experts.shape[0]
    part_width = tokens.shape[1]
    sharers = lax.axis_size("etp")
    my_part = lax.axis_index("etp")
    expert_count = up_weight.shape[0] * lax.axis_size("expert")
    capacity = 2 * tok_rows // expert_count * 11 // 8
    up_slab = up_weight[0]
    down_slab = down_weight[0]
    relative = experts ^ lax.axis_index("expert")
    slot_ids = slot_table(relative, expert_count, capacity)
    slots = jnp.arange(expert_count * capacity, dtype=jnp.int32)
    hits = slot_ids[:, :, None] == slots[None, None, :]
    placing = jnp.sum(hits.astype(jnp.bfloat16), axis=1)
    weights = jnp.sum(jnp.where(hits, mixing[:, :, None], 0.0), axis=1)
    coarse = weights.astype(jnp.bfloat16)
    fine = (weights - coarse.astype(jnp.float32)).astype(jnp.bfloat16)

    arrived = []
    for s in range(expert_count):
        rows = slice(s * capacity, (s + 1) * capacity)
        chunk = jnp.einsum(
            "rs,rd->sd", placing[:, rows], tokens, preferred_element_type=jnp.float32
        ).astype(jnp.bfloat16)
        arrived.append(swap(chunk, "expert", s) if s else chunk)

    half = expert_count // 2
    mixed = jnp.zeros((tok_rows, part_width), jnp.float32)
    for group in (range(half), range(half, expert_count)):
        full = jnp.zeros((half * capacity, sharers * part_width), jnp.bfloat16)
        for place, s in enumerate(group):
            for t in range(sharers):
                piece = swap(arrived[s], "etp", t) if t else arrived[s]
                full = lax.dynamic_update_slice(
                    full, piece, (place * capacity, (my_part ^ t) * part_width)
                )
        up_proj = jnp.dot(full, up_slab, preferred_element_type=jnp.float32)
        hidden = jax.nn.silu(up_proj).astype(jnp.bfloat16)
        sums = jnp.dot(hidden, down_slab, preferred_element_type=jnp.float32).astype(jnp.bfloat16)
        for place, s in reversed(list(enumerate(group))):
            own = None
            for t in range(sharers):
                piece = lax.dynamic_slice(
                    sums, (place * capacity, (my_part ^ t) * part_width), (capacity, part_width)
                )
                piece = (swap(piece, "etp", t) if t else piece).astype(jnp.float32)
                own = piece if own is None else own + piece
            own = own.astype(jnp.bfloat16)
            back = swap(own, "expert", s) if s else own
            rows = slice(s * capacity, (s + 1) * capacity)
            for share in (coarse, fine):
                mixed = mixed + jnp.dot(
                    share[:, rows], back, preferred_element_type=jnp.float32
                )
    return mixed.astype(jnp.bfloat16)


def solution(mesh):
    placed = (
        P(("dp", "expert"), "etp"),
        P(("dp", "expert"), None),
        P(("dp", "expert"), None),
        P("expert", None, "etp"),
        P("expert", "etp", None),
    )
    return jax.shard_map(
        local, mesh=mesh, in_specs=placed, out_specs=P(("dp", "expert"), "etp"), check_vma=False
    )
```

```python
import functools

import jax
import jax.numpy as jnp
from jax import lax
from jax.experimental import pallas as pl
from jax.experimental.pallas import tpu as pltpu
from jax.sharding import PartitionSpec as P

MESH = pl.DeviceIdType.MESH


def flipped(index, shift, count):
    total, bit = 0, 1
    while bit < count:
        digit = lax.rem(lax.div(index, bit), 2)
        total = total + (1 - digit if shift & bit else digit) * bit
        bit *= 2
    return total


def layer_kernel(
    chunks, sharers, tile,
    tok_ref, up_ref, down_ref, out_ref,
    up_v, down_v, full, hidden, other, own, landed,
    up_sem, down_sem, local_sem,
    zs_sem, zr_sem, ys_sem, yr_sem, bs_sem, br_sem, os_sem, or_sem,
):
    width = tok_ref.shape[2]
    units = up_v.shape[1]
    my_z = lax.axis_index("expert")
    my_y = lax.axis_index("etp")
    z_peer = [{"expert": flipped(my_z, s, chunks)} for s in range(chunks)]
    y_index = [flipped(my_y, t, sharers) for t in range(sharers)]
    y_peer = [{"etp": y_index[t]} for t in range(sharers)]

    def remote(src, dst, send, recv, peer):
        return pltpu.make_async_remote_copy(
            src_ref=src, dst_ref=dst, send_sem=send, recv_sem=recv,
            device_id=peer, device_id_type=MESH,
        )

    def columns(t):
        return pl.ds(t * width, width)

    up_copy, down_copy = [], []
    for t in range(sharers):
        begin = pl.multiple_of(y_index[t] * width, 128)
        up_copy.append(
            pltpu.make_async_copy(
                up_ref.at[pl.ds(begin, width), :], up_v.at[columns(t), :], up_sem.at[t]
            )
        )
        down_copy.append(
            pltpu.make_async_copy(
                down_ref.at[:, pl.ds(begin, width)], down_v.at[:, columns(t)], down_sem.at[t]
            )
        )
    first = pltpu.make_async_copy(tok_ref.at[0], full.at[0, :, columns(0)], local_sem.at[0])

    barrier = pltpu.get_barrier_semaphore()
    for peer in z_peer[1:] + y_peer[1:]:
        pl.semaphore_signal(barrier, inc=1, device_id=peer, device_id_type=MESH)
    pl.semaphore_wait(barrier, chunks - 1 + sharers - 1)

    z_go = [None] + [
        remote(
            tok_ref.at[s], full.at[s, :, columns(0)], zs_sem.at[s], zr_sem.at[s], z_peer[s]
        )
        for s in range(1, chunks)
    ]
    y_go = [
        [
            remote(
                full.at[s, :, columns(0)] if s else tok_ref.at[0],
                full.at[s, :, columns(t)], ys_sem.at[s, t], yr_sem.at[s, t], y_peer[t],
            )
            for t in range(1, sharers)
        ]
        for s in range(chunks)
    ]
    y_back = [
        [
            remote(
                other.at[s, t - 1], landed.at[s, t - 1], bs_sem.at[s, t], br_sem.at[s, t],
                y_peer[t],
            )
            for t in range(1, sharers)
        ]
        for s in range(chunks)
    ]
    z_back = [None] + [
        remote(own.at[s], out_ref.at[s], os_sem.at[s], or_sem.at[s], z_peer[s])
        for s in range(1, chunks)
    ]
    last = pltpu.make_async_copy(own.at[0], out_ref.at[0], local_sem.at[1])

    for copy in y_go[0]:
        copy.start()
    for s in range(1, chunks):
        z_go[s].start()
    first.start()
    for copy in up_copy + down_copy:
        copy.start()

    def forward(s):
        z_go[s].wait_recv()
        for copy in y_go[s]:
            copy.start()

    def up(s):
        @pl.loop(0, units // tile)
        def _(i):
            at = pl.ds(pl.multiple_of(i * tile, tile), tile)
            value = jnp.dot(full[s], up_v[:, at], preferred_element_type=jnp.float32)
            hidden[:, at] = (value / (1.0 + jnp.exp(-value))).astype(jnp.bfloat16)

    def down(s, t):
        target = other.at[s, t - 1] if t else own.at[s]

        @pl.loop(0, width // tile)
        def _(i):
            at = pl.multiple_of(i * tile, tile)
            value = jnp.dot(
                hidden[...], down_v[:, pl.ds(t * width + at, tile)],
                preferred_element_type=jnp.float32,
            )
            target[:, pl.ds(at, tile)] = value.astype(jnp.bfloat16)

    def start_back(s):
        for copy in y_back[s]:
            copy.start()

    def finish(s):
        for copy in y_back[s]:
            copy.wait_recv()
        total = own[s].astype(jnp.float32)
        for t in range(1, sharers):
            total = total + landed[s, t - 1].astype(jnp.float32)
        own[s] = total.astype(jnp.bfloat16)
        (z_back[s] if s else last).start()

    half = chunks // 2
    forward(1)
    first.wait()
    for s in range(chunks):
        if s >= 2 and s + 1 < chunks:
            forward(s + 1)
        for copy in y_go[s]:
            copy.wait_recv()
        if s == 0:
            for copy in up_copy:
                copy.wait()
        up(s)
        if s == 1 and chunks > 2:
            forward(2)
        if s == 0:
            for copy in down_copy:
                copy.wait()
        for t in range(1, sharers):
            down(s, t)
        if s == 0 or s >= half:
            start_back(s)
        down(s, 0)
    for s in range(1, half):
        start_back(s)
    for s in list(range(half, chunks)) + list(range(half)):
        finish(s)

    last.wait()
    for s in range(chunks):
        for copy in y_go[s] + y_back[s]:
            copy.wait_send()
        if s:
            z_go[s].wait_send()
            z_back[s].wait_send()
            z_back[s].wait_recv()


def run_layer(outgoing, up_slab, down_slab, sharers):
    chunks, capacity, width = outgoing.shape
    model, units = up_slab.shape
    tile = 512 if width % 512 == 0 else 256
    bf16 = jnp.bfloat16
    dma = pltpu.SemaphoreType.DMA
    anywhere = pl.BlockSpec(memory_space=pl.ANY)
    return pl.pallas_call(
        functools.partial(layer_kernel, chunks, sharers, tile),
        out_shape=jax.ShapeDtypeStruct(outgoing.shape, bf16),
        in_specs=[anywhere] * 3,
        out_specs=anywhere,
        scratch_shapes=[
            pltpu.VMEM((model, units), bf16),
            pltpu.VMEM((units, model), bf16),
            pltpu.VMEM((chunks, capacity, model), bf16),
            pltpu.VMEM((capacity, units), bf16),
            pltpu.VMEM((chunks, sharers - 1, capacity, width), bf16),
            pltpu.VMEM((chunks, capacity, width), bf16),
            pltpu.VMEM((chunks, sharers - 1, capacity, width), bf16),
            dma((sharers,)), dma((sharers,)), dma((2,)),
            dma((chunks,)), dma((chunks,)),
            dma((chunks, sharers)), dma((chunks, sharers)),
            dma((chunks, sharers)), dma((chunks, sharers)),
            dma((chunks,)), dma((chunks,)),
        ],
        compiler_params=pltpu.CompilerParams(
            collective_id=0, has_side_effects=True, vmem_limit_bytes=67_043_328
        ),
    )(outgoing, up_slab, down_slab)


def slot_table(chosen, expert_count, capacity):
    flat_ids = chosen.reshape(-1)
    one_hot = (flat_ids[:, None] == jnp.arange(expert_count, dtype=jnp.int32)[None, :]).astype(
        jnp.int32
    )
    before = jnp.cumsum(one_hot, axis=0) - one_hot
    position = jnp.sum(before * one_hot, axis=1)
    return (flat_ids * capacity + position).reshape(chosen.shape)


def local(tokens, experts, mixing, up_weight, down_weight):
    tok_rows = experts.shape[0]
    part_width = tokens.shape[1]
    sharers = lax.axis_size("etp")
    expert_count = up_weight.shape[0] * lax.axis_size("expert")
    capacity = 2 * tok_rows // expert_count * 11 // 8
    slot_total = expert_count * capacity
    relative = experts ^ lax.axis_index("expert")
    slot_ids = slot_table(relative, expert_count, capacity)
    slots = jnp.arange(slot_total, dtype=jnp.int32)
    hits = slot_ids[:, :, None] == slots[None, None, :]
    placing = jnp.sum(hits.astype(jnp.bfloat16), axis=1)
    outgoing = jnp.einsum(
        "rs,rd->sd", placing, tokens, preferred_element_type=jnp.float32
    ).astype(jnp.bfloat16)
    outputs = run_layer(
        outgoing.reshape(expert_count, capacity, part_width), up_weight[0], down_weight[0], sharers
    ).reshape(slot_total, part_width)
    weights = jnp.sum(jnp.where(hits, mixing[:, :, None], 0.0), axis=1)
    coarse = weights.astype(jnp.bfloat16)
    fine = (weights - coarse.astype(jnp.float32)).astype(jnp.bfloat16)
    mixed = jnp.dot(coarse, outputs, preferred_element_type=jnp.float32) + jnp.dot(
        fine, outputs, preferred_element_type=jnp.float32
    )
    return mixed.astype(jnp.bfloat16)


def solution(mesh):
    placed = (
        P(("dp", "expert"), "etp"),
        P(("dp", "expert"), None),
        P(("dp", "expert"), None),
        P("expert", None, "etp"),
        P("expert", "etp", None),
    )
    return jax.shard_map(
        local, mesh=mesh, in_specs=placed, out_specs=P(("dp", "expert"), "etp"), check_vma=False
    )
```

```python
import functools

import jax
import jax.numpy as jnp
from jax import lax
from jax.experimental import pallas as pl
from jax.experimental.pallas import tpu as pltpu
from jax.sharding import PartitionSpec as P

MESH = pl.DeviceIdType.MESH


def flipped(index, shift, count):
    total, bit = 0, 1
    while bit < count:
        digit = lax.rem(lax.div(index, bit), 2)
        total = total + (1 - digit if shift & bit else digit) * bit
        bit *= 2
    return total


def layer_kernel(
    chunks, sharers, tile,
    tok_ref, experts_ref, mixing_ref, up_ref, down_ref, out_ref, share_ref,
    up_v, down_v, full, hidden, other, own, landed, share_v,
    up_sem, down_sem, local_sem,
    zs_sem, zr_sem, ys_sem, yr_sem, bs_sem, br_sem, os_sem, or_sem,
):
    rows, width = tok_ref.shape
    capacity = full.shape[1]
    units = up_v.shape[1]
    my_z = lax.axis_index("expert")
    my_y = lax.axis_index("etp")
    z_index = [flipped(my_z, s, chunks) for s in range(chunks)]
    z_peer = [{"expert": z_index[s]} for s in range(chunks)]
    y_index = [flipped(my_y, t, sharers) for t in range(sharers)]
    y_peer = [{"etp": y_index[t]} for t in range(sharers)]
    cut = -(-capacity // 32) * 16
    pieces = [pl.ds(0, cut), pl.ds(cut, capacity - cut)]
    both = range(len(pieces))

    def remote(src, dst, send, recv, peer):
        return pltpu.make_async_remote_copy(
            src_ref=src, dst_ref=dst, send_sem=send, recv_sem=recv,
            device_id=peer, device_id_type=MESH,
        )

    def columns(t):
        return pl.ds(t * width, width)

    up_copy, down_copy = [], []
    for t in range(sharers):
        begin = pl.multiple_of(y_index[t] * width, 128)
        up_copy.append(
            pltpu.make_async_copy(
                up_ref.at[pl.ds(begin, width), :], up_v.at[columns(t), :], up_sem.at[t]
            )
        )
        down_copy.append(
            pltpu.make_async_copy(
                down_ref.at[:, pl.ds(begin, width)], down_v.at[:, columns(t)], down_sem.at[t]
            )
        )
    for copy in up_copy + down_copy:
        copy.start()

    barrier = pltpu.get_barrier_semaphore()
    for peer in z_peer[1:] + y_peer[1:]:
        pl.semaphore_signal(barrier, inc=1, device_id=peer, device_id_type=MESH)

    z_go = [None] + [
        [
            remote(
                own.at[s, piece], full.at[s, piece, columns(0)],
                zs_sem.at[s, p], zr_sem.at[s, p], z_peer[s],
            )
            for p, piece in enumerate(pieces)
        ]
        for s in range(1, chunks)
    ]
    y_go = [
        [
            [
                remote(
                    full.at[s, piece, columns(0)], full.at[s, piece, columns(t)],
                    ys_sem.at[s, t, p], yr_sem.at[s, t, p], y_peer[t],
                )
                for t in range(1, sharers)
            ]
            for p, piece in enumerate(pieces)
        ]
        for s in range(chunks)
    ]
    y_back = [
        [
            [
                remote(
                    other.at[s, t - 1, piece], landed.at[s, t - 1, piece],
                    bs_sem.at[s, t, p], br_sem.at[s, t, p], y_peer[t],
                )
                for t in range(1, sharers)
            ]
            for p, piece in enumerate(pieces)
        ]
        for s in range(chunks)
    ]
    z_back = [
        pltpu.make_async_copy(own.at[0, piece], out_ref.at[0, piece], local_sem.at[p])
        for p, piece in enumerate(pieces)
    ]
    z_back = [z_back] + [
        [
            remote(
                own.at[s, piece], out_ref.at[s, piece], os_sem.at[s, p], or_sem.at[s, p],
                z_peer[s],
            )
            for p, piece in enumerate(pieces)
        ]
        for s in range(1, chunks)
    ]
    share_copy = pltpu.make_async_copy(share_v, share_ref, local_sem.at[len(pieces)])

    lanes = lax.broadcasted_iota(jnp.int32, (rows, 128), 1)
    named = [experts_ref[:, k : k + 1] for k in range(2)]
    hot = [jnp.where(lanes == named[k], 1.0, 0.0) for k in range(2)]
    above = jnp.where(
        lax.broadcasted_iota(jnp.int32, (rows, rows), 0)
        > lax.broadcasted_iota(jnp.int32, (rows, rows), 1),
        1.0, 0.0,
    ).astype(jnp.bfloat16)
    counts = [
        jnp.dot(above, hot[k].astype(jnp.bfloat16), preferred_element_type=jnp.float32)
        for k in range(2)
    ]
    counts[1] = counts[1] + jnp.sum(hot[0], axis=0, keepdims=True)
    place = [jnp.sum(counts[k] * hot[k], axis=1, keepdims=True) for k in range(2)]

    def dispatch(s):
        slots = lax.broadcasted_iota(jnp.int32, (rows, capacity), 1).astype(jnp.float32)
        hit = jnp.zeros((rows, capacity), jnp.float32)
        for k in range(2):
            mine = jnp.where(named[k] == z_index[s], place[k], -1.0)
            hit = hit + jnp.where(slots == mine, 1.0, 0.0)
        chunk = lax.dot_general(
            hit.astype(jnp.bfloat16), tok_ref[...], (((0,), (0,)), ((), ())),
            preferred_element_type=jnp.float32,
        ).astype(jnp.bfloat16)
        if s:
            own[s] = chunk
        else:
            full[0, :, columns(0)] = chunk

    def forward(s, p):
        z_go[s][p].wait_recv()
        for copy in y_go[s][p]:
            copy.start()

    def up(s):
        @pl.loop(0, units // tile)
        def _(i):
            at = pl.ds(pl.multiple_of(i * tile, tile), tile)
            value = jnp.dot(full[s], up_v[:, at], preferred_element_type=jnp.float32)
            hidden[:, at] = (value / (1.0 + jnp.exp(-value))).astype(jnp.bfloat16)

    def down(s, t):
        target = other.at[s, t - 1] if t else own.at[s]

        @pl.loop(0, width // tile)
        def _(i):
            at = pl.multiple_of(i * tile, tile)
            value = jnp.dot(
                hidden[...], down_v[:, pl.ds(t * width + at, tile)],
                preferred_element_type=jnp.float32,
            )
            target[:, pl.ds(at, tile)] = value.astype(jnp.bfloat16)

    def start_back(s):
        for p in both:
            for copy in y_back[s][p]:
                copy.start()

    def finish(s, p):
        for copy in y_back[s][p]:
            copy.wait_recv()
        total = own[s, pieces[p]].astype(jnp.float32)
        for t in range(1, sharers):
            total = total + landed[s, t - 1, pieces[p]].astype(jnp.float32)
        own[s, pieces[p]] = total.astype(jnp.bfloat16)
        z_back[s][p].start()

    half = chunks // 2
    order = [0, half] + list(range(1, half)) + list(range(half + 1, chunks))
    dispatch(half)
    pl.semaphore_wait(barrier, chunks - 1 + sharers - 1)
    for copy in z_go[half]:
        copy.start()
    for s in [0] + order[2:]:
        dispatch(s)
        for p in both:
            for copy in [z_go[s][p]] if s else y_go[0][p]:
                copy.start()

    slots = lax.broadcasted_iota(jnp.int32, share_v.shape, 1).astype(jnp.float32)
    share = jnp.zeros(share_v.shape, jnp.float32)
    for k in range(2):
        slot = place[k]
        for s in range(1, chunks):
            slot = slot + jnp.where(named[k] == z_index[s], 1.0 * s * capacity, 0.0)
        share = share + jnp.where(slots == slot, mixing_ref[:, k : k + 1], 0.0)
    share_v[...] = share.astype(jnp.bfloat16)
    share_copy.start()

    forward(half, 0)
    for i, s in enumerate(order):
        for p in both:
            for copy in y_go[s][p]:
                copy.wait_recv()
        if i == 0:
            for copy in up_copy:
                copy.wait()
        up(s)
        if i == 0:
            forward(half, 1)
            for copy in down_copy:
                copy.wait()
        elif i + 2 < chunks:
            forward(order[i + 2], 0)
        for t in range(1, sharers):
            down(s, t)
        if s >= half:
            start_back(s)
        if i == chunks - 1:
            for done in order[:-1]:
                if done >= half:
                    for p in both:
                        finish(done, p)
        if s:
            for copy in z_go[s]:
                copy.wait_send()
        down(s, 0)
        if i + 2 < chunks:
            for p in both[1 if i else 0 :]:
                forward(order[i + 2], p)
    rest = list(range(1, half)) + [0]
    for s in rest:
        start_back(s)
    for s in order[-1:] + rest:
        for p in both:
            finish(s, p)

    share_copy.wait()
    for s in range(chunks):
        for p in both:
            for copy in y_go[s][p] + y_back[s][p]:
                copy.wait_send()
            if s:
                z_back[s][p].wait_send()
                z_back[s][p].wait_recv()
            else:
                z_back[s][p].wait()


def run_layer(tokens, experts, mixing, up_slab, down_slab, chunks, capacity, sharers):
    rows, width = tokens.shape
    model, units = up_slab.shape
    tile = 512 if width % 512 == 0 else 256
    bf16 = jnp.bfloat16
    dma = pltpu.SemaphoreType.DMA
    anywhere = pl.BlockSpec(memory_space=pl.ANY)
    near = pl.BlockSpec(memory_space=pltpu.VMEM)
    return pl.pallas_call(
        functools.partial(layer_kernel, chunks, sharers, tile),
        out_shape=(
            jax.ShapeDtypeStruct((chunks, capacity, width), bf16),
            jax.ShapeDtypeStruct((rows, chunks * capacity), bf16),
        ),
        in_specs=[near] * 3 + [anywhere] * 2,
        out_specs=(anywhere, anywhere),
        scratch_shapes=[
            pltpu.VMEM((model, units), bf16),
            pltpu.VMEM((units, model), bf16),
            pltpu.VMEM((chunks, capacity, model), bf16),
            pltpu.VMEM((capacity, units), bf16),
            pltpu.VMEM((chunks, sharers - 1, capacity, width), bf16),
            pltpu.VMEM((chunks, capacity, width), bf16),
            pltpu.VMEM((chunks, sharers - 1, capacity, width), bf16),
            pltpu.VMEM((rows, chunks * capacity), bf16),
            dma((sharers,)), dma((sharers,)), dma((3,)),
            dma((chunks, 2)), dma((chunks, 2)),
            dma((chunks, sharers, 2)), dma((chunks, sharers, 2)),
            dma((chunks, sharers, 2)), dma((chunks, sharers, 2)),
            dma((chunks, 2)), dma((chunks, 2)),
        ],
        compiler_params=pltpu.CompilerParams(
            collective_id=0, has_side_effects=True, vmem_limit_bytes=67_043_328
        ),
    )(tokens, experts, mixing, up_slab, down_slab)


def local(tokens, experts, mixing, up_weight, down_weight):
    tok_rows, part_width = tokens.shape
    sharers = lax.axis_size("etp")
    expert_count = up_weight.shape[0] * lax.axis_size("expert")
    capacity = 2 * tok_rows // expert_count * 11 // 8
    outputs, share = run_layer(
        tokens, experts, mixing, up_weight[0], down_weight[0], expert_count, capacity, sharers
    )
    outputs = outputs.reshape(expert_count * capacity, part_width)
    return jnp.dot(share, outputs, preferred_element_type=jnp.float32).astype(jnp.bfloat16)


def solution(mesh):
    placed = (
        P(("dp", "expert"), "etp"),
        P(("dp", "expert"), None),
        P(("dp", "expert"), None),
        P("expert", None, "etp"),
        P("expert", "etp", None),
    )
    return jax.shard_map(
        local, mesh=mesh, in_specs=placed, out_specs=P(("dp", "expert"), "etp"), check_vma=False
    )
```

```python
import functools

import jax
import jax.numpy as jnp
from jax import lax
from jax.experimental import pallas as pl
from jax.experimental.pallas import tpu as pltpu
from jax.sharding import PartitionSpec as P

MESH = pl.DeviceIdType.MESH


def flipped(index, shift, count):
    total, bit = 0, 1
    while bit < count:
        digit = lax.rem(lax.div(index, bit), 2)
        total = total + (1 - digit if shift & bit else digit) * bit
        bit *= 2
    return total


def layer_kernel(
    chunks, sharers, tile,
    tok_ref, routes_ref, up_ref, down_ref, out_ref, share_ref,
    up_v, down_v, full, hidden, other, own, landed, share_v,
    up_sem, down_sem, local_sem,
    zs_sem, zr_sem, ys_sem, yr_sem, bs_sem, br_sem, os_sem, or_sem,
):
    rows, width = tok_ref.shape
    capacity = full.shape[1]
    units = up_v.shape[1]
    my_z = lax.axis_index("expert")
    my_y = lax.axis_index("etp")
    z_index = [flipped(my_z, s, chunks) for s in range(chunks)]
    z_peer = [{"expert": z_index[s]} for s in range(chunks)]
    y_index = [flipped(my_y, t, sharers) for t in range(sharers)]
    y_peer = [{"etp": y_index[t]} for t in range(sharers)]
    cut = -(-capacity // 32) * 16
    pieces = [pl.ds(0, cut), pl.ds(cut, capacity - cut)]
    both = range(len(pieces))

    def remote(src, dst, send, recv, peer):
        return pltpu.make_async_remote_copy(
            src_ref=src, dst_ref=dst, send_sem=send, recv_sem=recv,
            device_id=peer, device_id_type=MESH,
        )

    def columns(t):
        return pl.ds(t * width, width)

    up_copy, down_copy = [], []
    for t in range(sharers):
        begin = pl.multiple_of(y_index[t] * width, 128)
        up_copy.append(
            pltpu.make_async_copy(
                up_ref.at[pl.ds(begin, width), :], up_v.at[columns(t), :], up_sem.at[t]
            )
        )
        down_copy.append(
            pltpu.make_async_copy(
                down_ref.at[:, pl.ds(begin, width)], down_v.at[:, columns(t)], down_sem.at[t]
            )
        )
    for copy in up_copy + down_copy:
        copy.start()

    barrier = pltpu.get_barrier_semaphore()
    for peer in z_peer[1:] + y_peer[1:]:
        pl.semaphore_signal(barrier, inc=1, device_id=peer, device_id_type=MESH)

    z_go = [None] + [
        [
            remote(
                own.at[s, piece], full.at[s, piece, columns(0)],
                zs_sem.at[s, p], zr_sem.at[s, p], z_peer[s],
            )
            for p, piece in enumerate(pieces)
        ]
        for s in range(1, chunks)
    ]
    y_go = [
        [
            [
                remote(
                    full.at[s, piece, columns(0)], full.at[s, piece, columns(t)],
                    ys_sem.at[s, t, p], yr_sem.at[s, t, p], y_peer[t],
                )
                for t in range(1, sharers)
            ]
            for p, piece in enumerate(pieces)
        ]
        for s in range(chunks)
    ]
    y_back = [
        [
            [
                remote(
                    other.at[s, t - 1, piece], landed.at[s, t - 1, piece],
                    bs_sem.at[s, t, p], br_sem.at[s, t, p], y_peer[t],
                )
                for t in range(1, sharers)
            ]
            for p, piece in enumerate(pieces)
        ]
        for s in range(chunks)
    ]
    z_back = [
        pltpu.make_async_copy(own.at[0, piece], out_ref.at[0, piece], local_sem.at[p])
        for p, piece in enumerate(pieces)
    ]
    z_back = [z_back] + [
        [
            remote(
                own.at[s, piece], out_ref.at[s, piece], os_sem.at[s, p], or_sem.at[s, p],
                z_peer[s],
            )
            for p, piece in enumerate(pieces)
        ]
        for s in range(1, chunks)
    ]
    share_copy = pltpu.make_async_copy(share_v, share_ref, local_sem.at[len(pieces)])

    lanes = lax.broadcasted_iota(jnp.int32, (rows, 128), 1).astype(jnp.float32)
    routes = jnp.transpose(routes_ref[...])
    named = [routes[:, k : k + 1] for k in range(2)]
    mixing = [routes[:, k : k + 1] for k in range(2, 4)]
    z_name = [z_index[s].astype(jnp.float32) for s in range(chunks)]
    hot = [jnp.where(lanes == named[k], 1.0, 0.0) for k in range(2)]
    above = jnp.where(
        lax.broadcasted_iota(jnp.int32, (rows, rows), 0)
        > lax.broadcasted_iota(jnp.int32, (rows, rows), 1),
        1.0, 0.0,
    ).astype(jnp.bfloat16)
    counts = [
        jnp.dot(above, hot[k].astype(jnp.bfloat16), preferred_element_type=jnp.float32)
        for k in range(2)
    ]
    counts[1] = counts[1] + jnp.sum(hot[0], axis=0, keepdims=True)
    place = [jnp.sum(counts[k] * hot[k], axis=1, keepdims=True) for k in range(2)]

    def dispatch(s):
        slots = lax.broadcasted_iota(jnp.int32, (rows, capacity), 1).astype(jnp.float32)
        hit = jnp.zeros((rows, capacity), jnp.float32)
        for k in range(2):
            mine = jnp.where(named[k] == z_name[s], place[k], -1.0)
            hit = hit + jnp.where(slots == mine, 1.0, 0.0)
        chunk = lax.dot_general(
            hit.astype(jnp.bfloat16), tok_ref[...], (((0,), (0,)), ((), ())),
            preferred_element_type=jnp.float32,
        ).astype(jnp.bfloat16)
        if s:
            own[s] = chunk
        else:
            full[0, :, columns(0)] = chunk

    def forward(s, p):
        z_go[s][p].wait_recv()
        for copy in y_go[s][p]:
            copy.start()

    def up(s):
        @pl.loop(0, units // tile)
        def _(i):
            at = pl.ds(pl.multiple_of(i * tile, tile), tile)
            value = jnp.dot(full[s], up_v[:, at], preferred_element_type=jnp.float32)
            hidden[:, at] = (value / (1.0 + jnp.exp(-value))).astype(jnp.bfloat16)

    def down(s, t):
        target = other.at[s, t - 1] if t else own.at[s]

        @pl.loop(0, width // tile)
        def _(i):
            at = pl.multiple_of(i * tile, tile)
            value = jnp.dot(
                hidden[...], down_v[:, pl.ds(t * width + at, tile)],
                preferred_element_type=jnp.float32,
            )
            target[:, pl.ds(at, tile)] = value.astype(jnp.bfloat16)

    def start_back(s):
        for p in both:
            for copy in y_back[s][p]:
                copy.start()

    def finish(s, p):
        for copy in y_back[s][p]:
            copy.wait_recv()
        total = own[s, pieces[p]].astype(jnp.float32)
        for t in range(1, sharers):
            total = total + landed[s, t - 1, pieces[p]].astype(jnp.float32)
        own[s, pieces[p]] = total.astype(jnp.bfloat16)
        z_back[s][p].start()

    half = chunks // 2
    order = list(range(chunks))
    dispatch(order[1])
    pl.semaphore_wait(barrier, chunks - 1 + sharers - 1)
    for copy in z_go[order[1]]:
        copy.start()
    for s in [0] + order[2:]:
        dispatch(s)
        for p in both:
            for copy in [z_go[s][p]] if s else y_go[0][p]:
                copy.start()

    slots = lax.broadcasted_iota(jnp.int32, share_v.shape, 1).astype(jnp.float32)
    share = jnp.zeros(share_v.shape, jnp.float32)
    for k in range(2):
        slot = place[k]
        for s in range(1, chunks):
            slot = slot + jnp.where(named[k] == z_name[s], 1.0 * s * capacity, 0.0)
        share = share + jnp.where(slots == slot, mixing[k], 0.0)
    share_v[...] = share.astype(jnp.bfloat16)
    share_copy.start()

    forward(order[1], 0)
    for i, s in enumerate(order):
        for p in both:
            for copy in y_go[s][p]:
                copy.wait_recv()
        if i == 0:
            for copy in up_copy:
                copy.wait()
        up(s)
        if i == 0:
            forward(order[1], 1)
            for copy in down_copy:
                copy.wait()
        elif i + 2 < chunks:
            forward(order[i + 2], 0)
        for t in range(1, sharers):
            down(s, t)
        if s >= half:
            start_back(s)
        if i == chunks - 1:
            for done in order[:-1]:
                if done >= half:
                    for p in both:
                        finish(done, p)
        if s:
            for copy in z_go[s]:
                copy.wait_send()
        down(s, 0)
        if i + 2 < chunks:
            for p in both[1 if i else 0 :]:
                forward(order[i + 2], p)
    rest = list(range(1, half)) + [0]
    for s in rest:
        start_back(s)
    for s in order[-1:] + rest:
        for p in both:
            finish(s, p)

    share_copy.wait()
    for s in range(chunks):
        for p in both:
            for copy in y_go[s][p] + y_back[s][p]:
                copy.wait_send()
            if s:
                z_back[s][p].wait_send()
                z_back[s][p].wait_recv()
            else:
                z_back[s][p].wait()


def run_layer(tokens, routes, up_slab, down_slab, chunks, capacity, sharers):
    rows, width = tokens.shape
    model, units = up_slab.shape
    tile = 512 if width % 512 == 0 else 256
    bf16 = jnp.bfloat16
    dma = pltpu.SemaphoreType.DMA
    anywhere = pl.BlockSpec(memory_space=pl.ANY)
    near = pl.BlockSpec(memory_space=pltpu.VMEM)
    return pl.pallas_call(
        functools.partial(layer_kernel, chunks, sharers, tile),
        out_shape=(
            jax.ShapeDtypeStruct((chunks, capacity, width), bf16),
            jax.ShapeDtypeStruct((rows, chunks * capacity), bf16),
        ),
        in_specs=[near] * 2 + [anywhere] * 2,
        out_specs=(anywhere, anywhere),
        scratch_shapes=[
            pltpu.VMEM((model, units), bf16),
            pltpu.VMEM((units, model), bf16),
            pltpu.VMEM((chunks, capacity, model), bf16),
            pltpu.VMEM((capacity, units), bf16),
            pltpu.VMEM((chunks, sharers - 1, capacity, width), bf16),
            pltpu.VMEM((chunks, capacity, width), bf16),
            pltpu.VMEM((chunks, sharers - 1, capacity, width), bf16),
            pltpu.VMEM((rows, chunks * capacity), bf16),
            dma((sharers,)), dma((sharers,)), dma((3,)),
            dma((chunks, 2)), dma((chunks, 2)),
            dma((chunks, sharers, 2)), dma((chunks, sharers, 2)),
            dma((chunks, sharers, 2)), dma((chunks, sharers, 2)),
            dma((chunks, 2)), dma((chunks, 2)),
        ],
        compiler_params=pltpu.CompilerParams(
            collective_id=0, has_side_effects=True, vmem_limit_bytes=67_043_328
        ),
    )(tokens, routes, up_slab, down_slab)


def local(tokens, experts, mixing, up_weight, down_weight):
    tok_rows, part_width = tokens.shape
    sharers = lax.axis_size("etp")
    expert_count = up_weight.shape[0] * lax.axis_size("expert")
    capacity = 2 * tok_rows // expert_count * 11 // 8
    routes = jnp.concatenate(
        [experts.T.astype(jnp.float32), mixing.T, jnp.zeros((4, tok_rows), jnp.float32)]
    )
    outputs, share = run_layer(
        tokens, routes, up_weight[0], down_weight[0], expert_count, capacity, sharers
    )
    outputs = outputs.reshape(expert_count * capacity, part_width)
    return jnp.dot(share, outputs, preferred_element_type=jnp.float32).astype(jnp.bfloat16)


def solution(mesh):
    placed = (
        P(("dp", "expert"), "etp"),
        P(("dp", "expert"), None),
        P(("dp", "expert"), None),
        P("expert", None, "etp"),
        P("expert", "etp", None),
    )
    return jax.shard_map(
        local, mesh=mesh, in_specs=placed, out_specs=P(("dp", "expert"), "etp"), check_vma=False
    )
```
